32 devices in a mesh: cells: 8 (over z, x), genes: 4 (over y, core).
Axes of the slice: x: 2, y: 2, z: 4, core: 2. Of those that a mesh axis runs over, the one named last changes fastest.
Arguments:
- expression: float32 [2048, 8192], P('cells', 'genes'), may hold values from 0.1 to 3000, as said below
- donor_label: int32 [2048], P('cells'), may hold values from 0 to 255
- live_count: int32 [8], P('cells'), may hold values from 16 to 256, as said below
- genotypes: bfloat16 [4, 8, 256, 4096], P('genes', 'cells'), may hold values from 0 to 2
- covariates: float32 [256, 2], replicated, may hold values from -4 to 4
- donor_cells: int32 [256], replicated, may hold values from 200 to 4999
- win_start: int32 [4, 2048], P('genes', 'cells'), may hold values from 0 to 2048
- win_len: int32 [4, 2048], P('genes', 'cells'), may hold values from 512 to 2048, as said below
Outputs:
- correlation: float32 [4, 2048, 4096], P('genes', 'cells')
- zscore_out: float32 [4, 2048, 256], P('genes', 'cells')
The draws below stay inside these ranges and needn't reach their ends.
Inputs may be any that keep to these rules, and one draw needn't show every extreme that they name: `live_count`: some index of cells has all 256 slots used. win_len[b0, k] is 2048 wherever k is a multiple of 256, so win_start + win_len <= 4096 throughout. `expression`: positive counts.
All inputs are finite; a program needn't handle non-finite values.
Results may differ from the reference program's by a relative error of at most 0.0003.
Values sent between devices are 32-bit elements; how exact they have to be, the bound alone decides.
A program may use at most 64 MiB of HBM per device.

```python
import jax
import jax.numpy as jnp
from jax import lax

G = 8192
VB = 4096
DONORS = 256
CAP = 256
CELLS = 2048
GCOL = 2048
GENE_BLK = 256
N_CELLS = 8
N_GENES = 4


def draw_expression(key, part):
    key_entry, key_gene, key_cell = jax.random.split(key, 3)
    column = jnp.arange(G, dtype=jnp.float32) / G
    entry = jnp.exp(jax.random.uniform(key_entry, (CELLS, G), jnp.float32, -2.0, 2.0))
    rising = jnp.exp(jnp.log(3.0) * column)
    gene_scale = jnp.exp(jax.random.uniform(key_gene, (G,), jnp.float32, 0.0, jnp.log(10.0))) * rising
    cell_scale = jnp.exp(jax.random.uniform(key_cell, (CELLS, 1), jnp.float32, 0.0, jnp.log(4.0)))
    return (entry * gene_scale[None, :] * cell_scale).astype(jnp.float32)


def draw_live_count(key, part):
    key_level, key_jitter, key_full = jax.random.split(key, 3)
    shifts = jax.random.randint(key_level, (N_CELLS,), 0, 4)
    highest = jnp.right_shift(jnp.full((N_CELLS,), CAP, jnp.int32), shifts.astype(jnp.int32))
    jitter = jax.random.randint(key_jitter, (N_CELLS,), 0, CAP // 16 + 1)
    counts = jnp.maximum(highest - jitter, 1)
    full_index = jax.random.randint(key_full, (), 0, N_CELLS)
    return jnp.where(jnp.arange(N_CELLS) == full_index, CAP, counts).astype(jnp.int32)


def window_pair(key):
    inner = jax.random.fold_in(key, 7)
    key_len, key_start = jax.random.split(inner)
    lengths = jax.random.randint(key_len, (N_GENES, GCOL), VB // 8, VB // 2 + 1)
    leading = (jnp.arange(GCOL) % GENE_BLK == 0)[None, :]
    lengths = jnp.where(leading, VB // 2, lengths)
    starts = jax.random.randint(key_start, (N_GENES, GCOL), 0, VB // 2 + 1)
    return (starts.astype(jnp.int32), lengths.astype(jnp.int32))


def draw_win_start(key, part):
    return window_pair(key)[0]


def draw_win_len(key, part):
    return window_pair(key)[1]


def touch_ends(entries, own_key, least, top_value):
    extent = entries.shape
    spot = [jax.random.randint(jax.random.fold_in(own_key, axis), (), 0, extent[axis]) for axis in range(len(extent))]
    entries = entries.at[tuple(spot)].set(least)
    longest = extent.index(max(extent))
    spot[longest] = (spot[longest] + 1) % extent[longest]
    return entries.at[tuple(spot)].set(top_value)


def levels(own_key, shape, cuts, smallest, largest):
    factor_of, own = 1.0, jax.random.fold_in(own_key, 6)
    for position, blocks in cuts:
        draws = jnp.exp(jax.random.uniform(jax.random.fold_in(own, position), (blocks,), jnp.float32, smallest / len(cuts), largest / len(cuts)))
        factor_of = factor_of * jnp.repeat(draws, shape[position] // blocks).reshape([-1 if axis == position else 1 for axis in range(len(shape))])
    return factor_of


def bell_draw(own_key, dims, spread, limit, held_as=jnp.bfloat16):
    values = jax.random.normal(own_key, dims, jnp.float32) * spread
    return jnp.minimum(jnp.maximum(values, -limit), limit).astype(held_as)


def setup_inputs(seed: int = 0) -> dict:
    streams_of = jax.random.split(jax.random.key(seed), 9)
    return {
        "expression": draw_expression(jax.random.fold_in(streams_of[8], 71), 0),
        "donor_label": touch_ends(jax.random.randint(streams_of[1], (CELLS,), 0, DONORS), jax.random.fold_in(streams_of[1], 1), 0, DONORS - 1).astype(jnp.int32),
        "live_count": draw_live_count(jax.random.fold_in(streams_of[8], 71), 0),
        "genotypes": jnp.clip(2.0 * jax.random.uniform(streams_of[3], (N_GENES, N_CELLS, DONORS, VB), jnp.float32) ** levels(streams_of[3], (N_GENES, N_CELLS, DONORS, VB), ((0, 4), (1, 8)), -0.2, 0.2), 0.0, 2.0).astype(jnp.bfloat16),
        "covariates": bell_draw(streams_of[4], (DONORS, 2), 1.0, 4.0, jnp.float32),
        "donor_cells": touch_ends(jax.random.randint(streams_of[5], (DONORS,), 200, 5000), jax.random.fold_in(streams_of[5], 1), 200, 4999).astype(jnp.int32),
        "win_start": draw_win_start(jax.random.fold_in(streams_of[8], 71), 0),
        "win_len": draw_win_len(jax.random.fold_in(streams_of[8], 71), 0),
    }


HIGHEST = lax.Precision.HIGHEST
epsilon = 1e-06
cpm_scale = 10000.0

def design_matrix(covariates, donor_cells):
    log_cells = jnp.log(donor_cells.astype(jnp.float32) / 1000.0)
    ones_col = jnp.ones((covariates.shape[0], 1), jnp.float32)
    return jnp.concatenate([ones_col, log_cells[:, None], covariates], axis=1)

def invert(gram_matrix):
    width = gram_matrix.shape[0]
    augmented = jnp.concatenate([gram_matrix, jnp.eye(width, dtype=jnp.float32)], axis=1)
    for pivot in range(width):
        pivot_row = augmented[pivot] / augmented[pivot, pivot]
        augmented = augmented - augmented[:, pivot][:, None] * pivot_row[None, :]
        augmented = augmented.at[pivot].set(pivot_row)
    return augmented[:, width:]

def reference(expression, donor_label, live_count, genotypes, covariates, donor_cells, win_start, win_len):
    cell_shards = expression.reshape(N_CELLS, CAP, G)
    label_shards = donor_label.reshape(N_CELLS, CAP)
    donor_ids = jnp.arange(DONORS, dtype=jnp.int32)
    slot_ids = jnp.arange(CAP, dtype=jnp.int32)

    def add_shard(running, pieces):
        shard_rows, labels, count = pieces
        onehot = ((labels[None, :] == donor_ids[:, None]) & (slot_ids < count)[None, :]).astype(jnp.float32)
        return (running + jnp.dot(onehot, shard_rows, precision=HIGHEST, preferred_element_type=jnp.float32), None)
    donor_sums, _ = lax.scan(add_shard, jnp.zeros((DONORS, G), jnp.float32), (cell_shards, label_shards, live_count))
    totals = lax.optimization_barrier(jnp.sum(donor_sums, axis=1))
    log_level = jnp.log1p(cpm_scale * donor_sums / (totals[:, None] + 1.0))
    design = design_matrix(covariates, donor_cells)
    gram_inv = invert(jnp.dot(design.T, design, precision=HIGHEST, preferred_element_type=jnp.float32))
    coeffs = jnp.dot(gram_inv, jnp.dot(design.T, log_level, precision=HIGHEST, preferred_element_type=jnp.float32), precision=HIGHEST, preferred_element_type=jnp.float32)
    residual = log_level - jnp.dot(design, coeffs, precision=HIGHEST, preferred_element_type=jnp.float32)
    zscore = residual * lax.rsqrt(lax.optimization_barrier(jnp.mean(residual * residual, axis=0, keepdims=True)) + epsilon)
    zscore_rows = zscore.T.reshape(N_GENES * N_CELLS, GENE_BLK, DONORS)
    dosage_blocks = genotypes.reshape(N_GENES * N_CELLS, DONORS, VB)
    starts = win_start.reshape(N_GENES * N_CELLS, GENE_BLK)
    lengths = win_len.reshape(N_GENES * N_CELLS, GENE_BLK)
    variant = jnp.arange(VB, dtype=jnp.int32)

    def one_block(pieces):
        dosage_bf, zrows, first, length = pieces
        dosage = dosage_bf.astype(jnp.float32)
        coef_x = jnp.dot(gram_inv, jnp.dot(design.T, dosage, precision=HIGHEST, preferred_element_type=jnp.float32), precision=HIGHEST, preferred_element_type=jnp.float32)
        dosage_res = dosage - jnp.dot(design, coef_x, precision=HIGHEST, preferred_element_type=jnp.float32)
        dosage_z = dosage_res * lax.rsqrt(lax.optimization_barrier(jnp.mean(dosage_res * dosage_res, axis=0, keepdims=True)) + epsilon)
        product = jnp.dot(zrows, dosage_z, precision=HIGHEST, preferred_element_type=jnp.float32) / DONORS
        inside = (variant[None, :] >= first[:, None]) & (variant[None, :] < (first + length)[:, None])
        return jnp.where(inside, product, jnp.float32(0.0))
    correlation = lax.map(one_block, (dosage_blocks, zscore_rows, starts, lengths))
    return (correlation.reshape(N_GENES, GCOL, VB), zscore_rows.reshape(N_GENES, GCOL, DONORS))
```

```python
import functools

import jax
import jax.numpy as jnp
from jax import lax
from jax.experimental import pallas as pl
from jax.experimental.pallas import tpu as pltpu
from jax.sharding import PartitionSpec as P

MESH = pl.DeviceIdType.MESH
epsilon = 1e-06
cpm_scale = 10000.0
SPLIT = 2


def halves(value):
    high = value.astype(jnp.bfloat16)
    low = (value - high.astype(jnp.float32)).astype(jnp.bfloat16)
    return high, low


def thirds(value):
    high = value.astype(jnp.bfloat16)
    rest = value - high.astype(jnp.float32)
    mid, low = halves(rest)
    return high, mid, low


def mm(left, right):
    return jnp.dot(left, right, preferred_element_type=jnp.float32)


def inverse_entries(rows):
    width = len(rows)
    gram = [[None] * width for _ in range(width)]
    for i in range(width):
        for j in range(i, width):
            gram[i][j] = jnp.sum(rows[i] * rows[j], axis=1, keepdims=True)
            gram[j][i] = gram[i][j]
    one = jnp.ones((1, 1), jnp.float32)
    zero = jnp.zeros((1, 1), jnp.float32)
    table = [gram[i] + [one if i == j else zero for j in range(width)] for i in range(width)]
    for pivot in range(width):
        top = [entry / table[pivot][pivot] for entry in table[pivot]]
        table = [
            top
            if i == pivot
            else [table[i][j] - table[i][pivot] * top[j] for j in range(2 * width)]
            for i in range(width)
        ]
    return [row[width:] for row in table]


def exchange_kernel(
    n_cells, n_genes,
    expr_hbm, label_ref, live_ref, geno_hbm, cov_ref, cells_ref,
    sums_ref, totals_ref, design_ref, scale_ref,
    expr, geno, onehot, part, xrecv, zrecv, tot_mine, tot_cells, tot_sum, tot_genes,
    load_sem, xs, xr, zs, zr, ts, tr, gs, gr,
):
    cap, local_genes = expr.shape
    donors = onehot.shape[1]
    lines = n_cells // 2
    blk = local_genes // n_cells
    piece = blk // SPLIT
    c = lax.axis_index("cells")
    gene_id = lax.axis_index("genes")
    a = c // 2
    b = lax.rem(c, 2)

    load_expr = pltpu.make_async_copy(expr_hbm, expr, load_sem.at[0])
    load_geno = pltpu.make_async_copy(geno_hbm.at[0, 0], geno, load_sem.at[1])
    load_expr.start()
    load_geno.start()

    barrier = pltpu.get_barrier_semaphore()

    def greet_cells(k, carry):
        pl.semaphore_signal(
            barrier, 1, device_id={"cells": lax.rem(c + k, n_cells)}, device_id_type=MESH
        )
        return carry

    lax.fori_loop(1, n_cells, greet_cells, 0)
    for k in range(1, n_genes):
        pl.semaphore_signal(
            barrier, 1, device_id={"genes": lax.rem(gene_id + k, n_genes)}, device_id_type=MESH
        )

    labels = label_ref[...]
    usable = lax.broadcasted_iota(jnp.int32, (1, cap), 1) < live_ref[0, 0]
    picked = jnp.where(usable, labels, -1)
    donor_ids = lax.broadcasted_iota(jnp.int32, (donors, cap), 0)
    spread = jnp.where(donor_ids == picked, 1.0, 0.0).astype(jnp.float32)
    spread = spread.T
    onehot[...] = spread.astype(jnp.bfloat16)

    load_expr.wait()
    per_cell = jnp.sum(expr[...], axis=1, keepdims=True)
    tot_mine[...] = jnp.sum(spread * per_cell, axis=0, keepdims=True)

    pl.semaphore_wait(barrier, n_cells - 1 + n_genes - 1)

    def send_total(k):
        return pltpu.make_async_remote_copy(
            tot_mine, tot_cells.at[k], ts.at[k], tr.at[k],
            device_id={"cells": lax.rem(c + k, n_cells)}, device_id_type=MESH,
        )

    def start_total(k, carry):
        send_total(k).start()
        return carry

    lax.fori_loop(1, n_cells, start_total, 0)

    def order(k):
        right, left = lines - 1 - a, a
        gap = jnp.abs(right - left)
        j = k - gap
        dist = jnp.minimum(right, left) - j // 2
        near = jnp.where(lax.rem(j, 2) == 0, a + dist, a - dist)
        far = jnp.where(right > left, lines - 1 - k, k)
        return jnp.where(k < gap, far, near)

    def multiply(start, width):
        high, low = halves(expr[:, pl.ds(pl.multiple_of(start, 128), width)])
        dims = (((0,), (0,)), ((), ()))
        hot = onehot[...]
        part[pl.ds(pl.multiple_of(start, 8), width), :] = lax.dot_general(
            high, hot, dims, preferred_element_type=jnp.float32
        ) + lax.dot_general(low, hot, dims, preferred_element_type=jnp.float32)

    def x_copy(d, s):
        row = pl.multiple_of((d * 2 + 1 - b) * blk + s * piece, 8)
        return pltpu.make_async_remote_copy(
            part.at[pl.ds(row, piece)], xrecv.at[d * SPLIT + s],
            xs.at[d * SPLIT + s], xr.at[d * SPLIT + s],
            device_id={"cells": a * 2 + 1 - b}, device_id_type=MESH,
        )

    aligned = blk % 128 == 0

    def send_x(k, carry):
        d = order(k)
        if aligned:
            multiply((d * 2 + 1 - b) * blk, blk)
        for s in range(SPLIT):
            x_copy(d, s).start()
        return carry

    if not aligned:
        wide = min(256, local_genes)

        def all_parts(j, carry):
            multiply(j * wide, wide)
            return carry

        lax.fori_loop(0, local_genes // wide, all_parts, 0)
    lax.fori_loop(0, lines, send_x, 0)
    if aligned:

        def own_part(k, carry):
            multiply((order(k) * 2 + b) * blk, blk)
            return carry

        lax.fori_loop(0, lines, own_part, 0)

    rows = [
        jnp.ones((1, donors), jnp.float32),
        jnp.log(cells_ref[...].astype(jnp.float32) / 1000.0),
        cov_ref[0:1, :],
        cov_ref[1:2, :],
    ]
    inverse = inverse_entries(rows)
    width = len(rows)
    solve = []
    for i in range(width):
        term = inverse[i][0] * rows[0]
        for j in range(1, width):
            term = term + inverse[i][j] * rows[j]
        solve.append(term)
    design_ref[...] = jnp.concatenate(rows + solve, axis=0)

    n_steps = lines * SPLIT
    variants = geno.shape[1]
    wide_v = 128
    while variants // wide_v > n_steps:
        wide_v *= 2
    chunks = variants // wide_v

    load_geno.wait()

    def dosage_chunk(t):
        both = design_ref[...]
        columns = both.T
        span = pl.ds(pl.multiple_of(t * wide_v, 128), wide_v)
        block = geno[:, span]
        p1, p2, p3 = thirds(both)
        coef = mm(p1, block) + mm(p2, block) + mm(p3, block)
        rest = block.astype(jnp.float32)
        for i in range(width):
            rest = rest - columns[:, i : i + 1] * coef[width + i : width + i + 1, :]
        scale_ref[:, span] = lax.rsqrt(
            jnp.mean(rest * rest, axis=0, keepdims=True) + epsilon
        ) / donors

    def z_copy(d, s, side, target):
        row = pl.multiple_of((d * 2 + b) * blk + s * piece, 8)
        slot = (side * lines + d) * SPLIT + s
        return pltpu.make_async_remote_copy(
            part.at[pl.ds(row, piece)], zrecv.at[slot],
            zs.at[d * SPLIT + s], zr.at[slot],
            device_id={"cells": target * 2 + b}, device_id_type=MESH,
        )

    def add_z(d, s, side, rows_of):
        z_copy(d, s, side, a).wait_recv()
        part[rows_of, :] = part[rows_of, :] + zrecv[(side * lines + d) * SPLIT + s]

    def send_genes(k):
        return pltpu.make_async_remote_copy(
            tot_sum, tot_genes.at[k], gs.at[k], gr.at[k],
            device_id={"genes": lax.rem(gene_id + k, n_genes)}, device_id_type=MESH,
        )

    def step(t, carry):
        @pl.when(t < chunks)
        def _():
            dosage_chunk(t)

        k, s = t // SPLIT, lax.rem(t, SPLIT)
        d = order(k)
        rows_of = pl.ds(pl.multiple_of((d * 2 + b) * blk + s * piece, 8), piece)
        x_copy(d, s).wait_recv()
        part[rows_of, :] = part[rows_of, :] + xrecv[d * SPLIT + s]

        @pl.when((d >= a) & (a > 0))
        def _():
            add_z(d, s, 0, rows_of)

        @pl.when((d <= a) & (a < lines - 1))
        def _():
            add_z(d, s, 1, rows_of)

        @pl.when(d > a)
        def _():
            z_copy(d, s, 0, a + 1).start()

        @pl.when(d < a)
        def _():
            z_copy(d, s, 1, a - 1).start()

        @pl.when(d == a)
        def _():
            sums_ref[pl.ds(pl.multiple_of(s * piece, 8), piece), :] = part[rows_of, :]

        @pl.when(t == 1)
        def _():
            def gather_total(k, running):
                send_total(k).wait_recv()
                return running + tot_cells[k]

            tot_sum[...] = lax.fori_loop(1, n_cells, gather_total, tot_mine[...])
            for k in range(1, n_genes):
                send_genes(k).start()

        return carry

    lax.fori_loop(0, n_steps, step, 0)

    total = tot_sum[...]
    for k in range(1, n_genes):
        send_genes(k).wait_recv()
        total = total + tot_genes[k]
    totals_ref[...] = total

    for k in range(1, n_genes):
        send_genes(k).wait_send()

    def drain_total(k, carry):
        send_total(k).wait_send()
        return carry

    lax.fori_loop(1, n_cells, drain_total, 0)

    def drain(t, carry):
        d, s = t // SPLIT, lax.rem(t, SPLIT)
        x_copy(d, s).wait_send()

        @pl.when(d != a)
        def _():
            z_copy(d, s, 0, a).wait_send()

        return carry

    lax.fori_loop(0, n_steps, drain, 0)


def correlate_kernel(
    sums_ref, totals_ref, design_ref, scale_ref, geno_ref, first_ref, length_ref,
    corr_ref, zscore_ref, z_high, z_low, low_end, high_end,
):
    blk, donors = sums_ref.shape
    wide = geno_ref.shape[3]
    width = design_ref.shape[0] // 2

    @pl.when(pl.program_id(0) == 0)
    def _():
        rows = [design_ref[i : i + 1, :] for i in range(2 * width)]

        def residual_of(level):
            coefs = [jnp.sum(level * rows[i], axis=1, keepdims=True) for i in range(width)]
            for i in range(width):
                level = level - coefs[i] * rows[width + i]
            return level

        level = jnp.log1p(cpm_scale * sums_ref[...] / (totals_ref[...] + 1.0))
        level = residual_of(level)
        zscore = level * lax.rsqrt(jnp.mean(level * level, axis=1, keepdims=True) + epsilon)
        zscore_ref[0] = zscore
        high, low = halves(residual_of(zscore))
        z_high[...] = high
        z_low[...] = low
        diagonal = lax.broadcasted_iota(jnp.int32, (blk, blk), 0) == lax.broadcasted_iota(
            jnp.int32, (blk, blk), 1
        )

        def column(row):
            held = jnp.where(diagonal, row.astype(jnp.float32), 0.0)
            return jnp.sum(held, axis=1, keepdims=True).astype(jnp.int32)

        first = column(first_ref[...])
        low_end[...] = first
        high_end[...] = first + column(length_ref[...])

    block = geno_ref[0, 0]
    product = (mm(z_high[...], block) + mm(z_low[...], block)) * scale_ref[...]
    variant = pl.program_id(0) * wide + lax.broadcasted_iota(jnp.int32, (1, wide), 1)
    inside = (variant >= low_end[...]) & (variant < high_end[...])
    corr_ref[0] = jnp.where(inside, product, 0.0)


def body(
    expression, donor_label, live_count, genotypes, covariates, donor_cells, win_start, win_len
):
    n_cells = lax.axis_size("cells")
    n_genes = lax.axis_size("genes")
    donors = covariates.shape[0]
    cap, local_genes = expression.shape
    blk = local_genes // n_cells
    variants = genotypes.shape[3]
    lines = n_cells // 2
    piece = blk // SPLIT
    f32, bf16 = jnp.float32, jnp.bfloat16
    vmem = pl.BlockSpec(memory_space=pltpu.VMEM)
    smem = pl.BlockSpec(memory_space=pltpu.SMEM)
    hbm = pl.BlockSpec(memory_space=pl.ANY)
    dma = pltpu.SemaphoreType.DMA
    sums, totals, design, scale = pl.pallas_call(
        functools.partial(exchange_kernel, n_cells, n_genes),
        out_shape=(
            jax.ShapeDtypeStruct((blk, donors), f32),
            jax.ShapeDtypeStruct((1, donors), f32),
            jax.ShapeDtypeStruct((8, donors), f32),
            jax.ShapeDtypeStruct((1, variants), f32),
        ),
        in_specs=[hbm, vmem, smem, hbm, vmem, vmem],
        out_specs=(vmem, vmem, vmem, vmem),
        scratch_shapes=[
            pltpu.VMEM((cap, local_genes), f32),
            pltpu.VMEM((donors, variants), bf16),
            pltpu.VMEM((cap, donors), bf16),
            pltpu.VMEM((local_genes, donors), f32),
            pltpu.VMEM((lines * SPLIT, piece, donors), f32),
            pltpu.VMEM((2 * lines * SPLIT, piece, donors), f32),
            pltpu.VMEM((1, donors), f32),
            pltpu.VMEM((n_cells, 1, donors), f32),
            pltpu.VMEM((1, donors), f32),
            pltpu.VMEM((n_genes, 1, donors), f32),
            dma((2,)),
            dma((lines * SPLIT,)),
            dma((lines * SPLIT,)),
            dma((lines * SPLIT,)),
            dma((2 * lines * SPLIT,)),
            dma((n_cells,)),
            dma((n_cells,)),
            dma((n_genes,)),
            dma((n_genes,)),
        ],
        compiler_params=pltpu.CompilerParams(
            collective_id=0, has_side_effects=True, vmem_limit_bytes=40 << 20
        ),
        name="exchange",
    )(
        expression,
        donor_label.reshape(1, cap),
        live_count.reshape(1, 1),
        genotypes,
        covariates.T,
        donor_cells.reshape(1, donors),
    )
    wide = min(1024, variants)
    whole = lambda shape: pl.BlockSpec(shape, lambda i: (0,) * len(shape))
    correlation, zscore = pl.pallas_call(
        correlate_kernel,
        grid=(variants // wide,),
        out_shape=(
            jax.ShapeDtypeStruct((1, blk, variants), f32),
            jax.ShapeDtypeStruct((1, blk, donors), f32),
        ),
        in_specs=[
            whole((blk, donors)),
            whole((1, donors)),
            whole((8, donors)),
            pl.BlockSpec((1, wide), lambda i: (0, i)),
            pl.BlockSpec((1, 1, donors, wide), lambda i: (0, 0, 0, i)),
            whole((1, blk)),
            whole((1, blk)),
        ],
        out_specs=(
            pl.BlockSpec((1, blk, wide), lambda i: (0, 0, i)),
            whole((1, blk, donors)),
        ),
        scratch_shapes=[
            pltpu.VMEM((blk, donors), bf16),
            pltpu.VMEM((blk, donors), bf16),
            pltpu.VMEM((blk, 1), jnp.int32),
            pltpu.VMEM((blk, 1), jnp.int32),
        ],
        name="correlate",
    )(sums, totals, design, scale, genotypes, win_start, win_len)
    return correlation, zscore


def solution(mesh):
    placed = (
        P("cells", "genes"),
        P("cells"),
        P("cells"),
        P("genes", "cells", None, None),
        P(),
        P(),
        P("genes", "cells"),
        P("genes", "cells"),
    )
    return jax.shard_map(
        body,
        mesh=mesh,
        in_specs=placed,
        out_specs=(P("genes", "cells", None), P("genes", "cells", None)),
        check_vma=False,
    )
```

```python
import functools

import jax
import jax.numpy as jnp
from jax import lax
from jax.experimental import pallas as pl
from jax.experimental.pallas import tpu as pltpu
from jax.sharding import PartitionSpec as P

MESH = pl.DeviceIdType.MESH
epsilon = 1e-06
cpm_scale = 10000.0


def halves(value):
    high = value.astype(jnp.bfloat16)
    low = (value - high.astype(jnp.float32)).astype(jnp.bfloat16)
    return high, low


def thirds(value):
    high = value.astype(jnp.bfloat16)
    rest = value - high.astype(jnp.float32)
    mid, low = halves(rest)
    return high, mid, low


def mm(left, right):
    return jnp.dot(left, right, preferred_element_type=jnp.float32)


def inverse_entries(rows):
    width = len(rows)
    gram = [[None] * width for _ in range(width)]
    for i in range(width):
        for j in range(i, width):
            gram[i][j] = jnp.sum(rows[i] * rows[j], axis=1, keepdims=True)
            gram[j][i] = gram[i][j]
    one = jnp.ones((1, 1), jnp.float32)
    zero = jnp.zeros((1, 1), jnp.float32)
    table = [gram[i] + [one if i == j else zero for j in range(width)] for i in range(width)]
    for pivot in range(width):
        top = [entry / table[pivot][pivot] for entry in table[pivot]]
        table = [
            top
            if i == pivot
            else [table[i][j] - table[i][pivot] * top[j] for j in range(2 * width)]
            for i in range(width)
        ]
    return [row[width:] for row in table]


def split_of(blk):
    return max(1, min(4, blk // 16))


def exchange_kernel(
    n_cells, n_genes,
    expr_hbm, label_ref, live_ref, geno_hbm, cov_ref, cells_ref,
    zscore_ref, high_ref, low_ref, scale_ref, geno,
    expr, design, columns, solve3, onehot, part, xrecv, zrecv, tot_mine, tot_cells, tot_sum, tot_genes, tot_all,
    load_sem, xs, xr, zs, zr, ts, tr, gs, gr,
):
    cap, local_genes = expr.shape
    donors = onehot.shape[1]
    lines = n_cells // 2
    blk = local_genes // n_cells
    split = split_of(blk)
    piece = blk // split
    aligned = blk % 128 == 0
    c = lax.axis_index("cells")
    gene_id = lax.axis_index("genes")
    a = c // 2
    b = lax.rem(c, 2)

    def order(k):
        right, left = lines - 1 - a, a
        gap = jnp.abs(right - left)
        j = k - gap
        dist = jnp.minimum(right, left) - j // 2
        near = jnp.where(lax.rem(j, 2) == 0, a + dist, a - dist)
        far = jnp.where(right > left, lines - 1 - k, k)
        return jnp.where(k < gap, far, near)

    load_geno = pltpu.make_async_copy(geno_hbm.at[0, 0], geno, load_sem.at[0])

    def load_expr(k):
        if not aligned:
            return pltpu.make_async_copy(expr_hbm, expr, load_sem.at[1])
        side = 1 - b if k < lines else b
        start = pl.multiple_of((order(k % lines) * 2 + side) * blk, 128)
        span = pl.ds(start, blk)
        return pltpu.make_async_copy(expr_hbm.at[:, span], expr.at[:, span], load_sem.at[1 + k])

    loads = n_cells if aligned else 1
    for k in range(loads):
        load_expr(k).start()

    barrier = pltpu.get_barrier_semaphore()

    def greet_cells(k, carry):
        pl.semaphore_signal(
            barrier, 1, device_id={"cells": lax.rem(c + k, n_cells)}, device_id_type=MESH
        )
        return carry

    lax.fori_loop(1, n_cells, greet_cells, 0)
    for k in range(1, n_genes):
        pl.semaphore_signal(
            barrier, 1, device_id={"genes": lax.rem(gene_id + k, n_genes)}, device_id_type=MESH
        )

    labels = label_ref[...]
    usable = lax.broadcasted_iota(jnp.int32, (1, cap), 1) < live_ref[0, 0]
    picked = jnp.where(usable, labels, -1)
    donor_ids = lax.broadcasted_iota(jnp.int32, (donors, cap), 0)
    spread = jnp.where(donor_ids == picked, 1.0, 0.0).astype(jnp.float32)
    spread = spread.T
    onehot[...] = spread.astype(jnp.bfloat16)

    def send_total(k):
        return pltpu.make_async_remote_copy(
            tot_mine, tot_cells.at[k], ts.at[k], tr.at[k],
            device_id={"cells": lax.rem(c + k, n_cells)}, device_id_type=MESH,
        )

    def start_total(k, carry):
        send_total(k).start()
        return carry

    def multiply(start, width):
        high, low = halves(expr[:, pl.ds(pl.multiple_of(start, 128), width)])
        dims = (((0,), (0,)), ((), ()))
        hot = onehot[...]
        part[pl.ds(pl.multiple_of(start, 8), width), :] = lax.dot_general(
            high, hot, dims, preferred_element_type=jnp.float32
        ) + lax.dot_general(low, hot, dims, preferred_element_type=jnp.float32)

    def x_copy(d, p):
        row = pl.multiple_of((d * 2 + 1 - b) * blk + p * piece, 8)
        return pltpu.make_async_remote_copy(
            part.at[pl.ds(row, piece)], xrecv.at[d * split + p],
            xs.at[d * split + p], xr.at[d * split + p],
            device_id={"cells": a * 2 + 1 - b}, device_id_type=MESH,
        )

    def send_x(k, carry):
        for p in range(split):
            x_copy(order(k), p).start()
        return carry

    def send_totals():
        per_cell = jnp.sum(expr[...], axis=1, keepdims=True)
        tot_mine[...] = jnp.sum(spread * per_cell, axis=0, keepdims=True)
        lax.fori_loop(1, n_cells, start_total, 0)

    def greeted():
        pl.semaphore_wait(barrier, n_cells - 1 + n_genes - 1)

    load_expr(0).wait()
    if aligned:

        def x_part(k, carry):
            multiply((order(k) * 2 + 1 - b) * blk, blk)
            return send_x(k, carry)

        def own_part(k, carry):
            multiply((order(k) * 2 + b) * blk, blk)
            return carry

        multiply((order(0) * 2 + 1 - b) * blk, blk)
        greeted()
        send_x(0, 0)
        for k in range(1, loads):
            load_expr(k).wait()
        load_geno.start()
        send_totals()
        lax.fori_loop(1, lines, x_part, 0)
        lax.fori_loop(0, lines, own_part, 0)
    else:
        wide = min(256, local_genes)

        def all_parts(j, carry):
            multiply(j * wide, wide)
            return carry

        load_geno.start()
        lax.fori_loop(0, local_genes // wide, all_parts, 0)
        greeted()
        send_totals()
        lax.fori_loop(0, lines, send_x, 0)

    rows = [
        jnp.ones((1, donors), jnp.float32),
        jnp.log(cells_ref[...].astype(jnp.float32) / 1000.0),
        cov_ref[0:1, :],
        cov_ref[1:2, :],
    ]
    inverse = inverse_entries(rows)
    width = len(rows)
    solve = []
    for i in range(width):
        term = inverse[i][0] * rows[0]
        for j in range(1, width):
            term = term + inverse[i][j] * rows[j]
        solve.append(term)
    both = jnp.concatenate(rows + solve, axis=0)
    design[...] = both
    columns[...] = both.T
    parts = [value.astype(jnp.float32) for value in thirds(both)]
    solve3[...] = jnp.concatenate(parts, axis=0).astype(jnp.bfloat16)

    n_steps = (lines - 1) * split
    variants = geno.shape[1]
    wide_v = 128
    while variants // wide_v > n_steps:
        wide_v *= 2
    chunks = variants // wide_v

    load_geno.wait()

    def dosage_chunk(t):
        span = pl.ds(pl.multiple_of(t * wide_v, 128), wide_v)
        block = geno[:, span]
        found = mm(solve3[...], block)
        coef = found[0:8] + found[8:16] + found[16:24]
        rest = block.astype(jnp.float32)
        for i in range(width):
            rest = rest - columns[:, i : i + 1] * coef[width + i : width + i + 1, :]
        scale_ref[:, span] = lax.rsqrt(
            jnp.mean(rest * rest, axis=0, keepdims=True) + epsilon
        ) / donors

    def z_copy(d, p, side, target):
        row = pl.multiple_of((d * 2 + b) * blk + p * piece, 8)
        slot = (side * lines + d) * split + p
        return pltpu.make_async_remote_copy(
            part.at[pl.ds(row, piece)], zrecv.at[slot],
            zs.at[d * split + p], zr.at[slot],
            device_id={"cells": target * 2 + b}, device_id_type=MESH,
        )

    def add_z(d, p, side, rows_of):
        z_copy(d, p, side, a).wait_recv()
        part[rows_of, :] = part[rows_of, :] + zrecv[(side * lines + d) * split + p]

    def send_genes(k):
        return pltpu.make_async_remote_copy(
            tot_sum, tot_genes.at[k], gs.at[k], gr.at[k],
            device_id={"genes": lax.rem(gene_id + k, n_genes)}, device_id_type=MESH,
        )

    def arrived(d, p):
        rows_of = pl.ds(pl.multiple_of((d * 2 + b) * blk + p * piece, 8), piece)
        x_copy(d, p).wait_recv()
        part[rows_of, :] = part[rows_of, :] + xrecv[d * split + p]

        @pl.when((d >= a) & (a > 0))
        def _():
            add_z(d, p, 0, rows_of)

        @pl.when((d <= a) & (a < lines - 1))
        def _():
            add_z(d, p, 1, rows_of)

        return rows_of

    def step(t, carry):
        @pl.when(t < chunks)
        def _():
            dosage_chunk(t)

        d, p = order(t // split), lax.rem(t, split)
        arrived(d, p)

        @pl.when(d > a)
        def _():
            z_copy(d, p, 0, a + 1).start()

        @pl.when(d < a)
        def _():
            z_copy(d, p, 1, a - 1).start()

        @pl.when(t == min(split, n_steps - 1))
        def _():
            def gather_total(k, running):
                send_total(k).wait_recv()
                return running + tot_cells[k]

            tot_sum[...] = lax.fori_loop(1, n_cells, gather_total, tot_mine[...])
            for k in range(1, n_genes):
                send_genes(k).start()

        return carry

    lax.fori_loop(0, n_steps, step, 0)

    total = tot_sum[...]
    for k in range(1, n_genes):
        send_genes(k).wait_recv()
        total = total + tot_genes[k]
    tot_all[...] = total

    def residual_of(level):
        coefs = [
            jnp.sum(level * design[i : i + 1, :], axis=1, keepdims=True) for i in range(width)
        ]
        for i in range(width):
            level = level - coefs[i] * design[width + i : width + i + 1, :]
        return level

    def own_piece(p, carry):
        rows_of = arrived(a, p)
        here = pl.ds(pl.multiple_of(p * piece, 16), piece)
        level = jnp.log1p(cpm_scale * part[rows_of, :] / (tot_all[...] + 1.0))
        level = residual_of(level)
        zscore = level * lax.rsqrt(jnp.mean(level * level, axis=1, keepdims=True) + epsilon)
        zscore_ref[here, :] = zscore
        high, low = halves(residual_of(zscore))
        high_ref[here, :] = high
        low_ref[here, :] = low
        return carry

    lax.fori_loop(0, split, own_piece, 0)

    for k in range(1, n_genes):
        send_genes(k).wait_send()

    def drain_total(k, carry):
        send_total(k).wait_send()
        return carry

    lax.fori_loop(1, n_cells, drain_total, 0)

    def drain(t, carry):
        d, p = order(t // split), lax.rem(t, split)
        x_copy(d, p).wait_send()

        @pl.when(t < n_steps)
        def _():
            z_copy(d, p, 0, a).wait_send()

        return carry

    lax.fori_loop(0, lines * split, drain, 0)


def correlate_kernel(
    zscore_in, z_high, z_low, scale_ref, geno_ref, first_ref, length_ref,
    corr_ref, zscore_ref, low_end, high_end,
):
    blk = z_high.shape[0]
    wide = corr_ref.shape[2]
    start = pl.multiple_of(pl.program_id(0) * wide, 128)

    @pl.when(pl.program_id(0) == 0)
    def _():
        zscore_ref[0] = zscore_in[...]
        diagonal = lax.broadcasted_iota(jnp.int32, (blk, blk), 0) == lax.broadcasted_iota(
            jnp.int32, (blk, blk), 1
        )

        def column(row):
            held = jnp.where(diagonal, row.astype(jnp.float32), 0.0)
            return jnp.sum(held, axis=1, keepdims=True).astype(jnp.int32)

        first = column(first_ref[...])
        low_end[...] = first
        high_end[...] = first + column(length_ref[...])

    block = geno_ref[:, pl.ds(start, wide)]
    product = mm(z_high[...], block) + mm(z_low[...], block)
    product = product * scale_ref[:, pl.ds(start, wide)]
    variant = start + lax.broadcasted_iota(jnp.int32, (1, wide), 1)
    inside = (variant >= low_end[...]) & (variant < high_end[...])
    corr_ref[0] = jnp.where(inside, product, 0.0)


def body(
    expression, donor_label, live_count, genotypes, covariates, donor_cells, win_start, win_len
):
    n_cells = lax.axis_size("cells")
    n_genes = lax.axis_size("genes")
    donors = covariates.shape[0]
    cap, local_genes = expression.shape
    blk = local_genes // n_cells
    variants = genotypes.shape[3]
    lines = n_cells // 2
    split = split_of(blk)
    piece = blk // split
    f32, bf16 = jnp.float32, jnp.bfloat16
    vmem = pl.BlockSpec(memory_space=pltpu.VMEM)
    smem = pl.BlockSpec(memory_space=pltpu.SMEM)
    hbm = pl.BlockSpec(memory_space=pltpu.HBM)
    dma = pltpu.SemaphoreType.DMA
    pinned = lambda value: pltpu.with_memory_space_constraint(value, pltpu.HBM)
    held = pl.pallas_call(
        functools.partial(exchange_kernel, n_cells, n_genes),
        out_shape=(
            pltpu.VMEM((blk, donors), f32),
            pltpu.VMEM((blk, donors), bf16),
            pltpu.VMEM((blk, donors), bf16),
            pltpu.VMEM((1, variants), f32),
            pltpu.VMEM((donors, variants), bf16),
        ),
        in_specs=[hbm, vmem, smem, hbm, vmem, vmem],
        out_specs=(vmem, vmem, vmem, vmem, vmem),
        scratch_shapes=[
            pltpu.VMEM((cap, local_genes), f32),
            pltpu.VMEM((8, donors), f32),
            pltpu.VMEM((donors, 8), f32),
            pltpu.VMEM((24, donors), bf16),
            pltpu.VMEM((cap, donors), bf16),
            pltpu.VMEM((local_genes, donors), f32),
            pltpu.VMEM((lines * split, piece, donors), f32),
            pltpu.VMEM((2 * lines * split, piece, donors), f32),
            pltpu.VMEM((1, donors), f32),
            pltpu.VMEM((n_cells, 1, donors), f32),
            pltpu.VMEM((1, donors), f32),
            pltpu.VMEM((n_genes, 1, donors), f32),
            pltpu.VMEM((1, donors), f32),
            dma((1 + n_cells,)),
            dma((lines * split,)),
            dma((lines * split,)),
            dma((lines * split,)),
            dma((2 * lines * split,)),
            dma((n_cells,)),
            dma((n_cells,)),
            dma((n_genes,)),
            dma((n_genes,)),
        ],
        compiler_params=pltpu.CompilerParams(
            collective_id=0, has_side_effects=True, vmem_limit_bytes=40 << 20
        ),
        name="exchange",
    )(
        pinned(expression),
        pinned(donor_label.reshape(1, cap)),
        live_count.reshape(1, 1),
        pinned(genotypes),
        pinned(covariates.T),
        pinned(donor_cells.reshape(1, donors)),
    )
    wide = min(1024, variants)
    whole = lambda shape: pl.BlockSpec(shape, lambda i: (0,) * len(shape))
    correlation, zscore = pl.pallas_call(
        correlate_kernel,
        grid=(variants // wide,),
        out_shape=(
            jax.ShapeDtypeStruct((1, blk, variants), f32),
            jax.ShapeDtypeStruct((1, blk, donors), f32),
        ),
        in_specs=[
            vmem,
            vmem,
            vmem,
            vmem,
            vmem,
            whole((1, blk)),
            whole((1, blk)),
        ],
        out_specs=(
            pl.BlockSpec((1, blk, wide), lambda i: (0, 0, i)),
            whole((1, blk, donors)),
        ),
        scratch_shapes=[
            pltpu.VMEM((blk, 1), jnp.int32),
            pltpu.VMEM((blk, 1), jnp.int32),
        ],
        compiler_params=pltpu.CompilerParams(vmem_limit_bytes=40 << 20),
        name="correlate",
    )(*held, win_start, win_len)
    return correlation, zscore


def solution(mesh):
    placed = (
        P("cells", "genes"),
        P("cells"),
        P("cells"),
        P("genes", "cells", None, None),
        P(),
        P(),
        P("genes", "cells"),
        P("genes", "cells"),
    )
    return jax.shard_map(
        body,
        mesh=mesh,
        in_specs=placed,
        out_specs=(P("genes", "cells", None), P("genes", "cells", None)),
        check_vma=False,
    )
```

```python
import functools

import jax
import jax.numpy as jnp
from jax import lax
from jax.experimental import pallas as pl
from jax.experimental.pallas import tpu as pltpu
from jax.sharding import PartitionSpec as P

MESH = pl.DeviceIdType.MESH
epsilon = 1e-06
cpm_scale = 10000.0


def halves(value):
    high = value.astype(jnp.bfloat16)
    low = (value - high.astype(jnp.float32)).astype(jnp.bfloat16)
    return high, low


def thirds(value):
    high = value.astype(jnp.bfloat16)
    rest = value - high.astype(jnp.float32)
    mid, low = halves(rest)
    return high, mid, low


def mm(left, right):
    return jnp.dot(left, right, preferred_element_type=jnp.float32)


def inverse_entries(rows):
    width = len(rows)
    gram = [[None] * width for _ in range(width)]
    for i in range(width):
        for j in range(i, width):
            gram[i][j] = jnp.sum(rows[i] * rows[j], axis=1, keepdims=True)
            gram[j][i] = gram[i][j]
    one = jnp.ones((1, 1), jnp.float32)
    zero = jnp.zeros((1, 1), jnp.float32)
    table = [gram[i] + [one if i == j else zero for j in range(width)] for i in range(width)]
    for pivot in range(width):
        top = [entry / table[pivot][pivot] for entry in table[pivot]]
        table = [
            top
            if i == pivot
            else [table[i][j] - table[i][pivot] * top[j] for j in range(2 * width)]
            for i in range(width)
        ]
    return [row[width:] for row in table]


def split_of(blk):
    return max(1, min(4, blk // 16))


def exchange_kernel(
    n_cells, n_genes,
    expr_hbm, label_ref, live_ref, geno_hbm, cov_ref, cells_ref,
    zscore_ref, high_ref, low_ref, scale_ref, geno,
    expr, design, columns, solve3, onehot, part, xrecv, zrecv, tot_mine, tot_cells, tot_sum, tot_genes, tot_all,
    load_sem, xs, xr, zs, zr, ts, tr, gs, gr,
):
    cap, local_genes = expr.shape
    donors = onehot.shape[1]
    lines = n_cells // 2
    blk = local_genes // n_cells
    split = split_of(blk)
    piece = blk // split
    aligned = blk % 128 == 0
    c = lax.axis_index("cells")
    gene_id = lax.axis_index("genes")
    a = c // 2
    b = lax.rem(c, 2)

    def order(k):
        right, left = lines - 1 - a, a
        gap = jnp.abs(right - left)
        j = k - gap
        dist = jnp.minimum(right, left) - j // 2
        near = jnp.where(lax.rem(j, 2) == 0, a + dist, a - dist)
        far = jnp.where(right > left, lines - 1 - k, k)
        return jnp.where(k < gap, far, near)

    load_geno = pltpu.make_async_copy(geno_hbm.at[0, 0], geno, load_sem.at[0])

    def load_expr(k):
        if not aligned:
            return pltpu.make_async_copy(expr_hbm, expr, load_sem.at[1])
        side = 1 - b if k < lines else b
        start = pl.multiple_of((order(k % lines) * 2 + side) * blk, 128)
        span = pl.ds(start, blk)
        return pltpu.make_async_copy(expr_hbm.at[:, span], expr.at[:, span], load_sem.at[1 + k])

    loads = n_cells if aligned else 1
    for k in range(loads):
        load_expr(k).start()

    barrier = pltpu.get_barrier_semaphore()

    def greet_cells(k, carry):
        pl.semaphore_signal(
            barrier, 1, device_id={"cells": lax.rem(c + k, n_cells)}, device_id_type=MESH
        )
        return carry

    lax.fori_loop(1, n_cells, greet_cells, 0)
    for k in range(1, n_genes):
        pl.semaphore_signal(
            barrier, 1, device_id={"genes": lax.rem(gene_id + k, n_genes)}, device_id_type=MESH
        )

    labels = label_ref[...]
    usable = lax.broadcasted_iota(jnp.int32, (1, cap), 1) < live_ref[0, 0]
    picked = jnp.where(usable, labels, -1)
    donor_ids = lax.broadcasted_iota(jnp.int32, (donors, cap), 0)
    spread = jnp.where(donor_ids == picked, 1.0, 0.0).astype(jnp.float32)
    spread = spread.T
    onehot[...] = spread.astype(jnp.bfloat16)

    def send_total(k):
        return pltpu.make_async_remote_copy(
            tot_mine, tot_cells.at[k], ts.at[k], tr.at[k],
            device_id={"cells": lax.rem(c + k, n_cells)}, device_id_type=MESH,
        )

    def start_total(k, carry):
        send_total(k).start()
        return carry

    def multiply(start, width):
        high, low = halves(expr[:, pl.ds(pl.multiple_of(start, 128), width)])
        dims = (((0,), (0,)), ((), ()))
        hot = onehot[...]
        part[pl.ds(pl.multiple_of(start, 8), width), :] = lax.dot_general(
            high, hot, dims, preferred_element_type=jnp.float32
        ) + lax.dot_general(low, hot, dims, preferred_element_type=jnp.float32)

    def x_copy(d, p):
        row = pl.multiple_of((d * 2 + 1 - b) * blk + p * piece, 8)
        return pltpu.make_async_remote_copy(
            part.at[pl.ds(row, piece)], xrecv.at[d * split + p],
            xs.at[d * split + p], xr.at[d * split + p],
            device_id={"cells": a * 2 + 1 - b}, device_id_type=MESH,
        )

    def send_x(k, carry):
        for p in range(split):
            x_copy(order(k), p).start()
        return carry

    def send_totals():
        per_cell = jnp.sum(expr[...], axis=1, keepdims=True)
        tot_mine[...] = jnp.sum(spread * per_cell, axis=0, keepdims=True)
        lax.fori_loop(1, n_cells, start_total, 0)

    def greeted():
        pl.semaphore_wait(barrier, n_cells - 1 + n_genes - 1)

    load_expr(0).wait()
    if aligned:

        def x_part(k, carry):
            multiply((order(k) * 2 + 1 - b) * blk, blk)
            return send_x(k, carry)

        def own_part(k, carry):
            multiply((order(k) * 2 + b) * blk, blk)
            return carry

        multiply((order(0) * 2 + 1 - b) * blk, blk)
        greeted()
        send_x(0, 0)
        for k in range(1, loads):
            load_expr(k).wait()
        load_geno.start()
        send_totals()
        lax.fori_loop(1, lines, x_part, 0)
        lax.fori_loop(0, lines, own_part, 0)
    else:
        wide = min(256, local_genes)

        def all_parts(j, carry):
            multiply(j * wide, wide)
            return carry

        load_geno.start()
        lax.fori_loop(0, local_genes // wide, all_parts, 0)
        greeted()
        send_totals()
        lax.fori_loop(0, lines, send_x, 0)

    rows = [
        jnp.ones((1, donors), jnp.float32),
        jnp.log(cells_ref[...].astype(jnp.float32) / 1000.0),
        cov_ref[0:1, :],
        cov_ref[1:2, :],
    ]
    inverse = inverse_entries(rows)
    width = len(rows)
    solve = []
    for i in range(width):
        term = inverse[i][0] * rows[0]
        for j in range(1, width):
            term = term + inverse[i][j] * rows[j]
        solve.append(term)
    both = jnp.concatenate(rows + solve, axis=0)
    design[...] = both
    columns[...] = both.T
    parts = [value.astype(jnp.float32) for value in thirds(both)]
    solve3[...] = jnp.concatenate(parts, axis=0).astype(jnp.bfloat16)

    n_steps = (lines - 1) * split
    variants = geno.shape[1]
    wide_v = 128
    while variants // wide_v > n_steps:
        wide_v *= 2
    chunks = variants // wide_v

    load_geno.wait()

    def dosage_chunk(t):
        span = pl.ds(pl.multiple_of(t * wide_v, 128), wide_v)
        block = geno[:, span]
        found = mm(solve3[...], block)
        coef = found[0:8] + found[8:16] + found[16:24]
        rest = block.astype(jnp.float32)
        for i in range(width):
            rest = rest - columns[:, i : i + 1] * coef[width + i : width + i + 1, :]
        scale_ref[:, span] = lax.rsqrt(
            jnp.mean(rest * rest, axis=0, keepdims=True) + epsilon
        ) / donors

    def z_copy(d, p, side, target):
        row = pl.multiple_of((d * 2 + b) * blk + p * piece, 8)
        slot = (side * lines + d) * split + p
        return pltpu.make_async_remote_copy(
            part.at[pl.ds(row, piece)], zrecv.at[slot],
            zs.at[d * split + p], zr.at[slot],
            device_id={"cells": target * 2 + b}, device_id_type=MESH,
        )

    def add_z(d, p, side, rows_of):
        z_copy(d, p, side, a).wait_recv()
        part[rows_of, :] = part[rows_of, :] + zrecv[(side * lines + d) * split + p]

    def send_genes(k):
        return pltpu.make_async_remote_copy(
            tot_sum, tot_genes.at[k], gs.at[k], gr.at[k],
            device_id={"genes": lax.rem(gene_id + k, n_genes)}, device_id_type=MESH,
        )

    def arrived(d, p):
        rows_of = pl.ds(pl.multiple_of((d * 2 + b) * blk + p * piece, 8), piece)
        x_copy(d, p).wait_recv()
        part[rows_of, :] = part[rows_of, :] + xrecv[d * split + p]

        @pl.when((d >= a) & (a > 0))
        def _():
            add_z(d, p, 0, rows_of)

        @pl.when((d <= a) & (a < lines - 1))
        def _():
            add_z(d, p, 1, rows_of)

        return rows_of

    def step(t, carry):
        @pl.when(t < chunks)
        def _():
            dosage_chunk(t)

        d, p = order(t // split), lax.rem(t, split)
        arrived(d, p)

        @pl.when(d > a)
        def _():
            z_copy(d, p, 0, a + 1).start()

        @pl.when(d < a)
        def _():
            z_copy(d, p, 1, a - 1).start()

        @pl.when(t == min(split, n_steps - 1))
        def _():
            def gather_total(k, running):
                send_total(k).wait_recv()
                return running + tot_cells[k]

            tot_sum[...] = lax.fori_loop(1, n_cells, gather_total, tot_mine[...])
            for k in range(1, n_genes):
                send_genes(k).start()

        return carry

    lax.fori_loop(0, n_steps, step, 0)

    total = tot_sum[...]
    for k in range(1, n_genes):
        send_genes(k).wait_recv()
        total = total + tot_genes[k]
    tot_all[...] = total

    def residual_of(level):
        coefs = [
            jnp.sum(level * design[i : i + 1, :], axis=1, keepdims=True) for i in range(width)
        ]
        for i in range(width):
            level = level - coefs[i] * design[width + i : width + i + 1, :]
        return level

    def own_piece(p, carry):
        rows_of = arrived(a, p)
        here = pl.ds(pl.multiple_of(p * piece, 16), piece)
        level = jnp.log1p(cpm_scale * part[rows_of, :] / (tot_all[...] + 1.0))
        level = residual_of(level)
        zscore = level * lax.rsqrt(jnp.mean(level * level, axis=1, keepdims=True) + epsilon)
        zscore_ref[here, :] = zscore
        high, low = halves(residual_of(zscore))
        high_ref[here, :] = high
        low_ref[here, :] = low
        return carry

    lax.fori_loop(0, split, own_piece, 0)

    for k in range(1, n_genes):
        send_genes(k).wait_send()

    def drain_total(k, carry):
        send_total(k).wait_send()
        return carry

    lax.fori_loop(1, n_cells, drain_total, 0)

    def drain(t, carry):
        d, p = order(t // split), lax.rem(t, split)
        x_copy(d, p).wait_send()

        @pl.when(t < n_steps)
        def _():
            z_copy(d, p, 0, a).wait_send()

        return carry

    lax.fori_loop(0, lines * split, drain, 0)


def correlate_kernel(
    zscore_in, z_high, z_low, scale_ref, geno_ref, first_ref, length_ref,
    corr_ref, zscore_ref, low_end, high_end,
):
    blk = z_high.shape[0]
    wide = corr_ref.shape[2]
    start = pl.multiple_of(pl.program_id(0) * wide, 128)

    @pl.when(pl.program_id(0) == 0)
    def _():
        zscore_ref[0] = zscore_in[...]
        diagonal = lax.broadcasted_iota(jnp.int32, (blk, blk), 0) == lax.broadcasted_iota(
            jnp.int32, (blk, blk), 1
        )

        def column(row):
            held = jnp.where(diagonal, row.astype(jnp.float32), 0.0)
            return jnp.sum(held, axis=1, keepdims=True).astype(jnp.int32)

        first = column(first_ref[...])
        low_end[...] = first
        high_end[...] = first + column(length_ref[...])

    block = geno_ref[:, pl.ds(start, wide)]
    product = mm(z_high[...], block) + mm(z_low[...], block)
    product = product * scale_ref[:, pl.ds(start, wide)]
    variant = start + lax.broadcasted_iota(jnp.int32, (1, wide), 1)
    inside = (variant >= low_end[...]) & (variant < high_end[...])
    corr_ref[0] = jnp.where(inside, product, 0.0)


def body(
    expression, donor_label, live_count, genotypes, covariates, donor_cells, win_start, win_len
):
    n_cells = lax.axis_size("cells")
    n_genes = lax.axis_size("genes")
    donors = covariates.shape[0]
    cap, local_genes = expression.shape
    blk = local_genes // n_cells
    variants = genotypes.shape[3]
    lines = n_cells // 2
    split = split_of(blk)
    piece = blk // split
    f32, bf16 = jnp.float32, jnp.bfloat16
    vmem = pl.BlockSpec(memory_space=pltpu.VMEM)
    smem = pl.BlockSpec(memory_space=pltpu.SMEM)
    hbm = pl.BlockSpec(memory_space=pltpu.HBM)
    dma = pltpu.SemaphoreType.DMA
    pinned = lambda value: pltpu.with_memory_space_constraint(value, pltpu.HBM)
    held = pl.pallas_call(
        functools.partial(exchange_kernel, n_cells, n_genes),
        out_shape=(
            pltpu.VMEM((blk, donors), f32),
            pltpu.VMEM((blk, donors), bf16),
            pltpu.VMEM((blk, donors), bf16),
            pltpu.VMEM((1, variants), f32),
            pltpu.VMEM((donors, variants), bf16),
        ),
        in_specs=[hbm, vmem, smem, hbm, vmem, vmem],
        out_specs=(vmem, vmem, vmem, vmem, vmem),
        scratch_shapes=[
            pltpu.VMEM((cap, local_genes), f32),
            pltpu.VMEM((8, donors), f32),
            pltpu.VMEM((donors, 8), f32),
            pltpu.VMEM((24, donors), bf16),
            pltpu.VMEM((cap, donors), bf16),
            pltpu.VMEM((local_genes, donors), f32),
            pltpu.VMEM((lines * split, piece, donors), f32),
            pltpu.VMEM((2 * lines * split, piece, donors), f32),
            pltpu.VMEM((1, donors), f32),
            pltpu.VMEM((n_cells, 1, donors), f32),
            pltpu.VMEM((1, donors), f32),
            pltpu.VMEM((n_genes, 1, donors), f32),
            pltpu.VMEM((1, donors), f32),
            dma((1 + n_cells,)),
            dma((lines * split,)),
            dma((lines * split,)),
            dma((lines * split,)),
            dma((2 * lines * split,)),
            dma((n_cells,)),
            dma((n_cells,)),
            dma((n_genes,)),
            dma((n_genes,)),
        ],
        compiler_params=pltpu.CompilerParams(
            collective_id=0, has_side_effects=True, vmem_limit_bytes=40 << 20
        ),
        name="exchange",
    )(
        pinned(expression),
        pinned(donor_label.reshape(1, cap)),
        live_count.reshape(1, 1),
        pinned(genotypes),
        pinned(covariates.T),
        pinned(donor_cells.reshape(1, donors)),
    )
    wide = min(512, variants)
    whole = lambda shape: pl.BlockSpec(shape, lambda i: (0,) * len(shape))
    correlation, zscore = pl.pallas_call(
        correlate_kernel,
        grid=(variants // wide,),
        out_shape=(
            jax.ShapeDtypeStruct((1, blk, variants), f32),
            jax.ShapeDtypeStruct((1, blk, donors), f32),
        ),
        in_specs=[
            vmem,
            vmem,
            vmem,
            vmem,
            vmem,
            whole((1, blk)),
            whole((1, blk)),
        ],
        out_specs=(
            pl.BlockSpec((1, blk, wide), lambda i: (0, 0, i)),
            whole((1, blk, donors)),
        ),
        scratch_shapes=[
            pltpu.VMEM((blk, 1), jnp.int32),
            pltpu.VMEM((blk, 1), jnp.int32),
        ],
        compiler_params=pltpu.CompilerParams(vmem_limit_bytes=40 << 20),
        name="correlate",
    )(*held, win_start, win_len)
    return correlation, zscore


def solution(mesh):
    placed = (
        P("cells", "genes"),
        P("cells"),
        P("cells"),
        P("genes", "cells", None, None),
        P(),
        P(),
        P("genes", "cells"),
        P("genes", "cells"),
    )
    return jax.shard_map(
        body,
        mesh=mesh,
        in_specs=placed,
        out_specs=(P("genes", "cells", None), P("genes", "cells", None)),
        check_vma=False,
    )
```
